32 devices in a mesh: expert: 8 (over z, core), row: 4 (over y, x).
Axes of the slice: x: 2, y: 2, z: 4, core: 2. Of those that a mesh axis runs over, the one named last changes fastest.
Arguments:
- grads: bfloat16 [8, 7168, 2048], P('expert', 'row')
- basis: bfloat16 [8, 7168, 256], P('expert', 'row'), may hold values from -0.0625 to 0.0625
- loads: int32 [8], P('expert'), may hold values from 1 to 1, as said below
- flags: int32 [8], P('expert'), may hold values 0 or 1
Outputs:
- new_basis: float32 [8, 7168, 256], P('expert', 'row')
- rotated: float32 [8, 256, 2048], P('expert', None, 'row')
The draws below stay inside these ranges and needn't reach their ends.
Inputs may be any that keep to these rules, and one draw needn't show every extreme that they name: Slots 0 to loads[d] - 1 of expert-axis index d are live and hold experts; the others are empty. Some index has all 1 slots live.
All inputs are finite; a program needn't handle non-finite values. No bound on the sum of `flags` on one device may be relied on, other than what follows from the above.
Results may differ from the reference program's by a relative error of at most 0.006.
Values sent between devices are 32-bit elements; how exact they have to be, the bound alone decides.
A program may use at most 64 MiB of HBM per device.

```python
import math
import jax
import jax.numpy as jnp
from jax import lax

D = 7168
S = 2048
K = 256
SLOTS = 1
EXPERTS = 8


def draw_grads(key, part):
    first_key, second_key = jax.random.split(jax.random.fold_in(key, 7))
    entries = jax.random.normal(first_key, (EXPERTS, D, S), jnp.float32)
    row_scale = jnp.exp(jax.random.uniform(second_key, (EXPERTS, D, 1), jnp.float32, math.log(0.5), math.log(5.0)))
    expert_ramp = 1.0 + 2.0 * jnp.arange(EXPERTS, dtype=jnp.float32) / max(EXPERTS - 1, 1)
    row_ramp = 1.0 + 2.0 * jnp.arange(D, dtype=jnp.float32) / (D - 1)
    factor = jnp.sqrt(expert_ramp)[:, None, None] * jnp.sqrt(row_ramp)[None, :, None]
    return (entries * row_scale * factor).astype(jnp.bfloat16)


def draw_loads(key, part):
    device_count = EXPERTS // SLOTS
    first_key, second_key = jax.random.split(jax.random.fold_in(key, 3))
    counts = jax.random.randint(first_key, (device_count,), 1, SLOTS + 1)
    chosen = jax.random.randint(second_key, (), 0, device_count)
    return jnp.where(jnp.arange(device_count) == chosen, SLOTS, counts).astype(jnp.int32)


def touch_ends(values, stream_key, smallest, high):
    extent = values.shape
    place = [jax.random.randint(jax.random.fold_in(stream_key, axis), (), 0, extent[axis]) for axis in range(len(extent))]
    values = values.at[tuple(place)].set(smallest)
    longest = extent.index(max(extent))
    place[longest] = (place[longest] + 1) % extent[longest]
    return values.at[tuple(place)].set(high)


def level_of(key, shape, cuts, smallest, top_value):
    factor_of, own = 1.0, jax.random.fold_in(key, 6)
    for axis_at, blocks in cuts:
        steps = jnp.exp(jax.random.uniform(jax.random.fold_in(own, axis_at), (blocks,), jnp.float32, smallest / len(cuts), top_value / len(cuts)))
        factor_of = factor_of * jnp.repeat(steps, shape[axis_at] // blocks).reshape([-1 if axis == axis_at else 1 for axis in range(len(shape))])
    return factor_of


def scatter_about(rng, shape, width, reach, cuts=(), kind=jnp.bfloat16):
    result = width * jax.random.normal(rng, shape, jnp.float32)
    if cuts:
        result = result * level_of(rng, shape, cuts, -0.22, 0.18)
    return jnp.clip(result, -reach, reach).astype(kind)


def setup_inputs(seed: int = 0) -> dict:
    streams_of = jax.random.split(jax.random.key(seed), 5)
    return {
        "grads": draw_grads(jax.random.fold_in(streams_of[4], 71), 0),
        "basis": scatter_about(streams_of[1], (EXPERTS, D, K), D ** -0.5, 0.0625, ((0, 8), (1, 4))),
        "loads": draw_loads(jax.random.fold_in(streams_of[4], 71), 0),
        "flags": touch_ends((jax.random.randint(streams_of[3], (EXPERTS,), 0, 2) < 1).astype(jnp.int32), jax.random.fold_in(streams_of[3], 1), 0, 1),
    }


def reference(grads, basis, loads, flags):
    expert_total = grads.shape[0]
    slot_count = expert_total // loads.shape[0]
    expert_ids = jnp.arange(expert_total, dtype=jnp.int32)
    live_mask = expert_ids % slot_count < loads[expert_ids // slot_count]
    refresh = jnp.logical_and(live_mask, flags == 1)

    def square_sum(expert):
        gradient = grads[expert].astype(jnp.float32)
        return jnp.sum(gradient * gradient)
    square_sums = lax.map(square_sum, expert_ids)
    total_sq = jnp.sum(jnp.where(live_mask, square_sums, 0.0))
    live_count = jnp.sum(live_mask.astype(jnp.float32))
    norm_scale = lax.rsqrt(total_sq / (live_count * D * S) + 1e-06)

    def refresh_one(expert):
        gradient = grads[expert]
        old_basis = basis[expert]
        inner_sum = jnp.dot(gradient.T.astype(jnp.float32), old_basis.astype(jnp.float32), preferred_element_type=jnp.float32).astype(jnp.bfloat16)
        power_rows = jnp.dot(gradient.astype(jnp.float32), inner_sum.astype(jnp.float32), preferred_element_type=jnp.float32).astype(jnp.bfloat16)
        ortho, upper = jnp.linalg.qr(power_rows.astype(jnp.float32))
        signs = jnp.where(jnp.diagonal(upper) < 0, -1.0, 1.0).astype(ortho.dtype)
        ortho = ortho * signs[None, :]
        fresh_rot = jnp.dot(ortho.T, gradient.astype(jnp.float32), precision=lax.Precision.HIGHEST)
        stale_rot = jnp.dot(old_basis.T.astype(jnp.float32), gradient.astype(jnp.float32), preferred_element_type=jnp.float32)
        basis_out = jnp.where(refresh[expert], ortho, jnp.where(live_mask[expert], old_basis.astype(jnp.float32), 0.0))
        rotated_out = jnp.where(refresh[expert], fresh_rot, jnp.where(live_mask[expert], stale_rot, 0.0)) * norm_scale
        return (basis_out, rotated_out)
    new_basis, rotated = lax.map(refresh_one, expert_ids)
    return (new_basis, rotated)
```

```python
import functools

import jax
import jax.numpy as jnp
from jax import lax
from jax.experimental import pallas as pl
from jax.experimental.pallas import tpu as pltpu
from jax.sharding import PartitionSpec as P

PANEL = 16
HIGHEST = lax.Precision.HIGHEST
F32 = jnp.float32
BF16 = jnp.bfloat16


def dot(a, b, precision=None):
    return lax.dot_general(a, b, (((1,), (0,)), ((), ())), precision=precision, preferred_element_type=F32)


def dot_t(a, b, precision=None):
    return lax.dot_general(a, b, (((1,), (1,)), ((), ())), precision=precision, preferred_element_type=F32)


def first_bit(mask, order):
    for phase, bit in enumerate(order):
        if mask >> bit & 1:
            return phase
    return len(order)


def panel_step(work, step):
    size = work.shape[0]
    panel = work[0:PANEL, :]
    rows = lax.broadcasted_iota(jnp.int32, (PANEL, 128), 0)
    lanes = lax.broadcasted_iota(jnp.int32, (PANEL, 128), 1)
    columns = [jnp.broadcast_to(panel[:, j : j + 1], (PANEL, 128)) for j in range(PANEL)]
    pieces = [panel[:, at : at + 128] for at in range(0, size, 128)]
    unit = (rows == lanes).astype(F32)
    root = jnp.zeros((PANEL, 128), F32)
    for j in range(PANEL):
        inverse_root = lax.rsqrt(columns[j][j : j + 1, :])
        root = jnp.where(rows == j, inverse_root, root)
        factor = jnp.where(rows > j, columns[j] * (inverse_root * inverse_root), 0.0)
        for k in range(j + 1, PANEL):
            columns[k] = columns[k] - factor * columns[k][j : j + 1, :]
        pieces = [piece - factor * piece[j : j + 1, :] for piece in pieces]
        unit = unit - factor * unit[j : j + 1, :]
    scaled = [root * piece for piece in pieces]
    full = jnp.concatenate([jnp.where(lanes < PANEL, root * unit, scaled[0])] + scaled[1:], axis=1)
    where = lax.broadcasted_iota(jnp.int32, (PANEL, size), 1)
    open_columns = jnp.logical_and(where >= PANEL, where < size - PANEL * step)
    left = jnp.where(open_columns, jnp.concatenate(scaled, axis=1), 0.0)
    update = dot(left.T, full, HIGHEST)
    body = work[PANEL:, :]
    ahead = lax.broadcasted_iota(jnp.int32, body.shape, 1) < PANEL
    rest = jnp.where(ahead, 0.0, body) - update[PANEL:, :]
    work[0 : size - PANEL, :] = pltpu.roll(rest, size - PANEL, 1)
    work[size - PANEL :, :] = pltpu.roll(full, size - PANEL, 1)


def panel_steps(work, begin, end):
    def body(step, carry):
        panel_step(work, step)
        return carry

    lax.fori_loop(begin, end, body, 0)


def lower_of(work):
    shape = work.shape
    below = lax.broadcasted_iota(jnp.int32, shape, 1) <= lax.broadcasted_iota(jnp.int32, shape, 0)
    return jnp.where(below, work[...], 0.0)


def kernel(
    n, experts, entries, g_ref, b_ref, live_ref, refresh_ref, fresh_ref, rot_ref,
    bt, part, land, part2, land2, full, inner, power, power_t, first, work, inv1,
    gram, gram_land, total, total_land,
    s_rs, r_rs, s_ag, r_ag, s_rs2, r_rs2, s_gr, r_gr, s_tot, r_tot,
):
    bits = n.bit_length() - 1
    expert_bits = experts.bit_length() - 1
    depth, wide = g_ref.shape
    size = b_ref.shape[1]
    half = size // 2
    block = wide // n
    me = lax.axis_index("row")
    my_expert = lax.axis_index("expert")
    orders = [tuple(range(bits)), tuple(reversed(range(bits)))]

    def other(index, mask):
        at = index
        for bit in range(max(bits, expert_bits)):
            if mask >> bit & 1:
                at = at + (1 - 2 * (lax.rem(index // (1 << bit), 2))) * (1 << bit)
        return at

    def partner(bit):
        return {"row": other(me, 1 << bit), "expert": my_expert}

    def expert_partner(bit):
        return {"row": me, "expert": other(my_expert, 1 << bit)}

    everyone = [partner(b) for b in range(bits)] + [expert_partner(b) for b in range(expert_bits)]
    barrier = pltpu.get_barrier_semaphore()
    for peer in everyone:
        pl.semaphore_signal(barrier, inc=1, device_id=peer, device_id_type=pl.DeviceIdType.MESH)

    def columns(mask):
        return pl.ds(pl.multiple_of(other(me, mask) * block, block), block)

    def copy(src, dst, send, recv, to):
        return pltpu.make_async_remote_copy(
            src_ref=src, dst_ref=dst, send_sem=send, recv_sem=recv,
            device_id=to, device_id_type=pl.DeviceIdType.MESH,
        )

    moves = []
    for phase in range(bits):
        for h in range(2):
            order = orders[h]
            masks = [m for m in range(n) if first_bit(m, order) == phase]
            masks.sort(key=lambda m: first_bit(m & ~(1 << order[phase]), order))
            moves.append([(h, phase, m, m & ~(1 << order[phase])) for m in masks])
    schedule = []
    for phase in range(bits):
        a, b = moves[2 * phase], moves[2 * phase + 1]
        schedule.append([move for pair in zip(a, b) for move in pair])
    slot = {}
    for phase_moves in schedule:
        for h, phase, m, there in phase_moves:
            slot[h, phase, there] = len(slot)

    def halving(part_ref, land_ref, sends, recvs):
        def make(h, phase, m, there):
            at = slot[h, phase, there]
            return copy(part_ref.at[h, m], land_ref.at[at], sends.at[at], recvs.at[at], partner(orders[h][phase]))

        def absorb(h, phase, m):
            at = slot[h, phase, m]
            back = m | 1 << orders[h][phase]
            make(h, phase, back, m).wait_recv()
            part_ref[h, m] = part_ref[h, m] + land_ref[at]

        return make, absorb

    def begin(left_ref, part_ref, make):
        started = set()
        for move in schedule[0]:
            h, _, m, _ = move
            part_ref[h, m] = dot(left_ref[h * half : (h + 1) * half, :], g_ref[:, columns(m)])
            make(*move).start()
            started.add((h, m))
        for m in range(n):
            for h in range(2):
                if (h, m) not in started:
                    part_ref[h, m] = dot(left_ref[h * half : (h + 1) * half, :], g_ref[:, columns(m)])

    def forward(make, absorb):
        for phase in range(1, bits):
            for move in schedule[phase]:
                h, _, m, _ = move
                for earlier in range(phase):
                    absorb(h, earlier, m)
                make(*move).start()

    def finish(make, absorb):
        for phase in range(bits):
            for h in range(2):
                absorb(h, phase, 0)
        for phase_moves in schedule:
            for move in phase_moves:
                make(*move).wait_send()

    def gram_exchange(use, between=None):
        for phase in range(bits):
            made = []
            for h in range(2):
                rows = slice(h * half, (h + 1) * half)
                made.append(copy(
                    gram.at[use, phase, rows], gram_land.at[use, phase, rows],
                    s_gr.at[use, phase, h], r_gr.at[use, phase, h], partner(orders[h][phase]),
                ))
            for item in made:
                item.start()
            if between is not None and phase == 0:
                between()
            for h, item in enumerate(made):
                rows = slice(h * half, (h + 1) * half)
                item.wait_recv()
                gram[use, phase + 1, rows] = gram[use, phase, rows] + gram_land[use, phase, rows]
            for item in made:
                item.wait_send()

    peers = everyone

    def total_copy(at):
        return copy(total.at[at], total_land.at[at], s_tot.at[at], r_tot.at[at], peers[at])

    def total_next(at):
        total_copy(at).wait()
        total[at + 1] = total[at] + total_land[at]
        if at + 1 < len(peers):
            total_copy(at + 1).start()

    live = live_ref[0] >= 1
    refresh = refresh_ref[0] == 1

    strip = 128 if depth % 128 == 0 else depth
    for at in range(0, depth, strip):
        bt[:, at : at + strip] = b_ref[at : at + strip, :].T

    pl.semaphore_wait(barrier, len(everyone))

    make, absorb = halving(part, land, s_rs, r_rs)
    begin(bt, part, make)

    def squares_of(step, sums):
        rows = g_ref[pl.ds(pl.multiple_of(step * 16, 16), 16), :].astype(F32)
        square = rows * rows
        for at in range(0, wide, 128):
            sums = sums + square[0:8, at : at + 128] + square[8:16, at : at + 128]
        return sums

    sums = lax.fori_loop(0, depth // 16, squares_of, jnp.zeros((8, 128), F32))
    total_sq = jnp.where(live, jnp.sum(sums), 0.0)
    count = jnp.where(jnp.logical_and(live, me == 0), 1.0, 0.0)
    tile_row = lax.broadcasted_iota(jnp.int32, (8, 128), 0)
    total[0] = jnp.where(tile_row == 0, total_sq, jnp.where(tile_row == 1, count, 0.0))
    total_copy(0).start()

    forward(make, absorb)
    finish(make, absorb)

    mine = jnp.concatenate([part[0, 0], part[1, 0]], axis=0).astype(BF16)
    gram[0, 0] = dot_t(mine, mine)
    gram_exchange(0)

    spread = []
    for h in range(2):
        order = tuple(reversed(orders[h]))
        held = [0]
        for bit in order:
            for m in list(held):
                spread.append((h, bit, m))
                held.append(m | 1 << bit)
    number = {(h, m | 1 << bit): at for at, (h, bit, m) in enumerate(spread)}

    def spread_copy(h, bit, m):
        at = number[h, m | 1 << bit]
        src = part.at[h, 0] if m == 0 else full.at[h, m]
        return copy(src, full.at[h, m | 1 << bit], s_ag.at[at], r_ag.at[at], partner(bit))

    arrived = set()

    def take(h, m):
        if m == 0 or (h, m) in arrived:
            return
        arrived.add((h, m))
        bit = next(b for (hh, b, mm) in spread if hh == h and mm | 1 << b == m)
        spread_copy(h, bit, m & ~(1 << bit)).wait_recv()

    def keep(h, m):
        source = part[h, 0] if m == 0 else full[h, m]
        inner[columns(m), h * half : (h + 1) * half] = source.T.astype(BF16)

    rank = {0: [], 1: []}
    for h, bit, m in spread:
        if m == 0:
            rank[h].append((h, bit, m))
    for pair in zip(rank[0], rank[1]):
        for item in pair:
            spread_copy(*item).start()
    work[...] = gram[0, bits]
    panels = size // PANEL
    panel_steps(work, 0, panels // 2)
    total_next(0)
    for h, bit, m in sorted((s for s in spread if s[2]), key=lambda s: bin(s[2]).count("1")):
        take(h, m)
        spread_copy(h, bit, m).start()
    panel_steps(work, panels // 2, panels)
    inv1[...] = lower_of(work)
    keep(0, 0)
    keep(1, 0)
    for m in sorted(range(1, n), key=lambda v: bin(v).count("1")):
        for h in range(2):
            take(h, m)
            keep(h, m)
    for item in spread:
        spread_copy(*item).wait_send()
    if len(peers) > 1:
        total_next(1)

    tile = 256 if depth % 256 == 0 else 64

    def power_rows(at):
        rows = slice(at, at + tile)
        power[rows, :] = dot(g_ref[rows, :], inner[...]).astype(BF16)
        power_t[:, rows] = power[rows, :].T

    for at in range(0, depth, tile):
        power_rows(at)
    first_t = dot(inv1[...], power_t[...].astype(F32), HIGHEST)
    gram[1, 0] = dot_t(first_t, first_t, HIGHEST)

    make2, absorb2 = halving(part2, land2, s_rs2, r_rs2)

    def beside():
        first[...] = dot_t(power[...].astype(F32), inv1[...], HIGHEST)

    gram_exchange(1, beside)
    begin(power_t, part2, make2)
    for at in range(2, len(peers) - 1):
        total_next(at)
    work[...] = gram[1, bits]
    panel_steps(work, 0, panels // 2)
    forward(make2, absorb2)
    panel_steps(work, panels // 2, panels)
    inv2 = lower_of(work)
    fresh = dot_t(first[...], inv2, HIGHEST)
    fresh_ref[...] = jnp.where(refresh, fresh, jnp.where(live, b_ref[...].astype(F32), 0.0))
    both = dot(inv2, inv1[...], HIGHEST)
    if len(peers) > 2:
        total_next(len(peers) - 1)
    final = total[len(peers)]
    norm = lax.rsqrt(final[0:1, 0:1] / (final[1:2, 0:1] * entries) + 1e-6)
    finish(make2, absorb2)
    cross = jnp.concatenate([part2[0, 0], part2[1, 0]], axis=0)
    stale = jnp.concatenate([part[0, 0], part[1, 0]], axis=0)
    turned = dot(both, cross, HIGHEST)
    rot_ref[...] = jnp.where(refresh, turned, jnp.where(live, stale, 0.0)) * norm


def on_device(n, experts, grads, basis, loads, flags):
    _, depth, wide = grads.shape
    size = basis.shape[2]
    block = wide // n
    bits = n.bit_length() - 1
    peers = bits + experts.bit_length() - 1
    moves = 2 * (n - 1)
    live = loads
    refresh = jnp.where(loads >= 1, flags, 0)
    vmem = pl.BlockSpec(memory_space=pltpu.VMEM)
    smem = pl.BlockSpec(memory_space=pltpu.SMEM)
    chunk = (size // 2, block)
    dma = pltpu.SemaphoreType.DMA
    new_basis, rotated = pl.pallas_call(
        functools.partial(kernel, n, experts, float(depth * n * wide)),
        out_shape=(
            jax.ShapeDtypeStruct((depth, size), F32),
            jax.ShapeDtypeStruct((size, block), F32),
        ),
        in_specs=[vmem, vmem, smem, smem],
        out_specs=(vmem, vmem),
        scratch_shapes=[
            pltpu.VMEM((size, depth), BF16),
            pltpu.VMEM((2, n, *chunk), F32),
            pltpu.VMEM((moves, *chunk), F32),
            pltpu.VMEM((2, n, *chunk), F32),
            pltpu.VMEM((moves, *chunk), F32),
            pltpu.VMEM((2, n, *chunk), F32),
            pltpu.VMEM((wide, size), BF16),
            pltpu.VMEM((depth, size), BF16),
            pltpu.VMEM((size, depth), BF16),
            pltpu.VMEM((depth, size), F32),
            pltpu.VMEM((size, size), F32),
            pltpu.VMEM((size, size), F32),
            pltpu.VMEM((2, bits + 1, size, size), F32),
            pltpu.VMEM((2, bits, size, size), F32),
            pltpu.VMEM((peers + 1, 8, 128), F32),
            pltpu.VMEM((peers, 8, 128), F32),
            dma((moves,)), dma((moves,)), dma((moves,)), dma((moves,)), dma((moves,)), dma((moves,)),
            dma((2, bits, 2)), dma((2, bits, 2)), dma((peers,)), dma((peers,)),
        ],
        compiler_params=pltpu.CompilerParams(
            collective_id=0, has_side_effects=True, vmem_limit_bytes=58 * 1024 * 1024
        ),
    )(grads[0], basis[0], live, refresh)
    return new_basis[None], rotated[None]


def solution(mesh):
    placed = (P("expert", "row", None), P("expert", "row", None), P("expert"), P("expert"))
    return jax.shard_map(
        functools.partial(on_device, mesh.shape["row"], mesh.shape["expert"]),
        mesh=mesh,
        in_specs=placed,
        out_specs=(P("expert", "row", None), P("expert", None, "row")),
        check_vma=False,
    )
```

```python
import functools

import jax
import jax.numpy as jnp
from jax import lax
from jax.experimental import pallas as pl
from jax.experimental.pallas import tpu as pltpu
from jax.sharding import PartitionSpec as P

PANEL = 16
HIGHEST = lax.Precision.HIGHEST
F32 = jnp.float32
BF16 = jnp.bfloat16


def dot(a, b, precision=None):
    return lax.dot_general(a, b, (((1,), (0,)), ((), ())), precision=precision, preferred_element_type=F32)


def dot_t(a, b, precision=None):
    return lax.dot_general(a, b, (((1,), (1,)), ((), ())), precision=precision, preferred_element_type=F32)


def pieces_of(x, count):
    pieces = []
    for _ in range(count):
        pieces.append(x.astype(BF16))
        x = x - pieces[-1].astype(F32)
    return pieces


def first_bit(mask, order):
    for phase, bit in enumerate(order):
        if mask >> bit & 1:
            return phase
    return len(order)


def panel_step(work, step):
    size = work.shape[0]
    panel = work[0:PANEL, :]
    rows = lax.broadcasted_iota(jnp.int32, (PANEL, 128), 0)
    lanes = lax.broadcasted_iota(jnp.int32, (PANEL, 128), 1)
    columns = [jnp.broadcast_to(panel[:, j : j + 1], (PANEL, 128)) for j in range(PANEL)]
    pieces = [panel[:, at : at + 128] for at in range(0, size, 128)]
    unit = (rows == lanes).astype(F32)
    root = jnp.zeros((PANEL, 128), F32)
    for j in range(PANEL):
        inverse_root = lax.rsqrt(columns[j][j : j + 1, :])
        root = jnp.where(rows == j, inverse_root, root)
        factor = jnp.where(rows > j, columns[j] * (inverse_root * inverse_root), 0.0)
        for k in range(j + 1, PANEL):
            columns[k] = columns[k] - factor * columns[k][j : j + 1, :]
        pieces = [piece - factor * piece[j : j + 1, :] for piece in pieces]
        unit = unit - factor * unit[j : j + 1, :]
    scaled = [root * piece for piece in pieces]
    full = jnp.concatenate([jnp.where(lanes < PANEL, root * unit, scaled[0])] + scaled[1:], axis=1)
    where = lax.broadcasted_iota(jnp.int32, (PANEL, size), 1)
    open_columns = jnp.logical_and(where >= PANEL, where < size - PANEL * step)
    left = jnp.where(open_columns, jnp.concatenate(scaled, axis=1), 0.0)
    update = dot(left.T, full, HIGHEST)
    body = work[PANEL:, :]
    ahead = lax.broadcasted_iota(jnp.int32, body.shape, 1) < PANEL
    rest = jnp.where(ahead, 0.0, body) - update[PANEL:, :]
    work[0 : size - PANEL, :] = pltpu.roll(rest, size - PANEL, 1)
    work[size - PANEL :, :] = pltpu.roll(full, size - PANEL, 1)


def panel_steps(work, begin, end):
    def body(step, carry):
        panel_step(work, step)
        return carry

    lax.fori_loop(begin, end, body, 0)


def lower_of(work):
    shape = work.shape
    below = lax.broadcasted_iota(jnp.int32, shape, 1) <= lax.broadcasted_iota(jnp.int32, shape, 0)
    return jnp.where(below, work[...], 0.0)


def kernel(
    n, experts, entries, g_hbm, b_ref, live_ref, refresh_ref, fresh_ref, rot_ref,
    g_ref, g_sem, bt, part, land, part2, land2, full, inner, power_t, rough, tops, lows, top_rows, low_rows, work, inv1,
    gram, gram_land, total, total_land,
    s_rs, r_rs, s_ag, r_ag, s_rs2, r_rs2, s_gr, r_gr, s_tot, r_tot,
):
    depth, wide = g_ref.shape
    bits = n.bit_length() - 1
    expert_bits = experts.bit_length() - 1
    size = b_ref.shape[1]
    half = size // 2
    block = wide // n
    me = lax.axis_index("row")
    my_expert = lax.axis_index("expert")
    orders = [tuple(range(bits)), tuple(reversed(range(bits)))]

    def other(index, mask):
        at = index
        for bit in range(max(bits, expert_bits)):
            if mask >> bit & 1:
                at = at + (1 - 2 * (lax.rem(index // (1 << bit), 2))) * (1 << bit)
        return at

    def partner(bit):
        return {"row": other(me, 1 << bit), "expert": my_expert}

    def expert_partner(bit):
        return {"row": me, "expert": other(my_expert, 1 << bit)}

    everyone = [partner(b) for b in range(bits)] + [expert_partner(b) for b in range(expert_bits)]
    barrier = pltpu.get_barrier_semaphore()
    for peer in everyone:
        pl.semaphore_signal(barrier, inc=1, device_id=peer, device_id_type=pl.DeviceIdType.MESH)

    def columns(mask):
        return pl.ds(pl.multiple_of(other(me, mask) * block, block), block)

    def load(mask):
        return pltpu.make_async_copy(g_hbm.at[:, columns(mask)], g_ref.at[:, columns(mask)], g_sem.at[mask])

    def copy(src, dst, send, recv, to):
        return pltpu.make_async_remote_copy(
            src_ref=src, dst_ref=dst, send_sem=send, recv_sem=recv,
            device_id=to, device_id_type=pl.DeviceIdType.MESH,
        )

    moves = []
    for phase in range(bits):
        for h in range(2):
            order = orders[h]
            masks = [m for m in range(n) if first_bit(m, order) == phase]
            masks.sort(key=lambda m: first_bit(m & ~(1 << order[phase]), order))
            moves.append([(h, phase, m, m & ~(1 << order[phase])) for m in masks])
    schedule = []
    for phase in range(bits):
        a, b = moves[2 * phase], moves[2 * phase + 1]
        schedule.append([move for pair in zip(a, b) for move in pair])
    slot = {}
    for phase_moves in schedule:
        for h, phase, m, there in phase_moves:
            slot[h, phase, there] = len(slot)

    def halving(part_ref, land_ref, sends, recvs):
        def make(h, phase, m, there):
            at = slot[h, phase, there]
            return copy(part_ref.at[h, m], land_ref.at[at], sends.at[at], recvs.at[at], partner(orders[h][phase]))

        def absorb(h, phase, m):
            at = slot[h, phase, m]
            back = m | 1 << orders[h][phase]
            make(h, phase, back, m).wait_recv()
            part_ref[h, m] = part_ref[h, m] + land_ref[at]

        return make, absorb

    def begin(left_ref, part_ref, make, ensure=lambda m: None):
        started = set()
        for move in schedule[0]:
            h, _, m, _ = move
            ensure(m)
            part_ref[h, m] = dot(left_ref[h * half : (h + 1) * half, :], g_ref[:, columns(m)])
            make(*move).start()
            started.add((h, m))
        for m in range(n):
            ensure(m)
            for h in range(2):
                if (h, m) not in started:
                    part_ref[h, m] = dot(left_ref[h * half : (h + 1) * half, :], g_ref[:, columns(m)])

    def forward(make, absorb):
        for phase in range(1, bits):
            for move in schedule[phase]:
                h, _, m, _ = move
                for earlier in range(phase):
                    absorb(h, earlier, m)
                make(*move).start()

    def finish(make, absorb):
        for phase in range(bits):
            for h in range(2):
                absorb(h, phase, 0)
        for phase_moves in schedule:
            for move in phase_moves:
                make(*move).wait_send()

    def gram_exchange(use, between=None):
        for phase in range(bits):
            made = []
            for h in range(2):
                rows = slice(h * half, (h + 1) * half)
                made.append(copy(
                    gram.at[use, phase, rows], gram_land.at[use, phase, rows],
                    s_gr.at[use, phase, h], r_gr.at[use, phase, h], partner(orders[h][phase]),
                ))
            for item in made:
                item.start()
            if between is not None:
                between(phase)
            for h, item in enumerate(made):
                rows = slice(h * half, (h + 1) * half)
                item.wait_recv()
                gram[use, phase + 1, rows] = gram[use, phase, rows] + gram_land[use, phase, rows]
            for item in made:
                item.wait_send()

    peers = everyone

    def total_copy(at):
        return copy(total.at[at], total_land.at[at], s_tot.at[at], r_tot.at[at], peers[at])

    def total_next(at):
        total_copy(at).wait()
        total[at + 1] = total[at] + total_land[at]
        if at + 1 < len(peers):
            total_copy(at + 1).start()

    make, absorb = halving(part, land, s_rs, r_rs)
    wanted = [move[2] for move in schedule[0]] + list(range(n))
    wanted = sorted(range(n), key=wanted.index)
    for m in wanted:
        load(m).start()

    live = live_ref[0] >= 1
    refresh = refresh_ref[0] == 1

    strip = 128 if depth % 128 == 0 else depth
    for at in range(0, depth, strip):
        bt[:, at : at + strip] = b_ref[at : at + strip, :].T

    pl.semaphore_wait(barrier, len(everyone))

    loaded = []

    def ensure(m):
        if m not in loaded:
            load(m).wait()
            loaded.append(m)

    begin(bt, part, make, ensure)

    def squares_of(step, sums):
        rows = g_ref[pl.ds(pl.multiple_of(step * 16, 16), 16), :].astype(F32)
        square = rows * rows
        for at in range(0, wide, 128):
            sums = sums + square[0:8, at : at + 128] + square[8:16, at : at + 128]
        return sums

    sums = lax.fori_loop(0, depth // 16, squares_of, jnp.zeros((8, 128), F32))
    total_sq = jnp.where(live, jnp.sum(sums), 0.0)
    count = jnp.where(jnp.logical_and(live, me == 0), 1.0, 0.0)
    tile_row = lax.broadcasted_iota(jnp.int32, (8, 128), 0)
    total[0] = jnp.where(tile_row == 0, total_sq, jnp.where(tile_row == 1, count, 0.0))
    total_copy(0).start()

    forward(make, absorb)
    finish(make, absorb)

    mine = jnp.concatenate([part[0, 0], part[1, 0]], axis=0).astype(BF16)
    gram[0, 0] = dot_t(mine, mine)
    gram_exchange(0)

    spread = []
    for h in range(2):
        order = tuple(reversed(orders[h]))
        held = [0]
        for bit in order:
            for m in list(held):
                spread.append((h, bit, m))
                held.append(m | 1 << bit)
    number = {(h, m | 1 << bit): at for at, (h, bit, m) in enumerate(spread)}

    def spread_copy(h, bit, m):
        at = number[h, m | 1 << bit]
        src = part.at[h, 0] if m == 0 else full.at[h, m]
        return copy(src, full.at[h, m | 1 << bit], s_ag.at[at], r_ag.at[at], partner(bit))

    arrived = set()

    def take(h, m):
        if m == 0 or (h, m) in arrived:
            return
        arrived.add((h, m))
        bit = next(b for (hh, b, mm) in spread if hh == h and mm | 1 << b == m)
        spread_copy(h, bit, m & ~(1 << bit)).wait_recv()

    def keep(h, m):
        source = part[h, 0] if m == 0 else full[h, m]
        inner[columns(m), h * half : (h + 1) * half] = source.T.astype(BF16)

    rank = {0: [], 1: []}
    for h, bit, m in spread:
        if m == 0:
            rank[h].append((h, bit, m))
    for pair in zip(rank[0], rank[1]):
        for item in pair:
            spread_copy(*item).start()
    work[...] = gram[0, bits]
    panels = size // PANEL
    panel_steps(work, 0, panels // 2)
    total_next(0)
    for h, bit, m in sorted((s for s in spread if s[2]), key=lambda s: bin(s[2]).count("1")):
        take(h, m)
        spread_copy(h, bit, m).start()
    panel_steps(work, panels // 2, panels)
    inv1[...] = lower_of(work)
    tile = 256 if depth % 256 == 0 else 64
    masks = sorted(range(n), key=lambda v: bin(v).count("1"))
    for m in masks:
        for h in range(2):
            take(h, m)
            keep(h, m)
        if m == masks[-1]:
            break
        for at in range(0, depth, tile):
            rows = slice(at, at + tile)
            term = dot(g_ref[rows, columns(m)], inner[columns(m), :])
            rough[rows, :] = term if m == 0 else rough[rows, :] + term
    for at in range(0, depth, tile):
        rows = slice(at, at + tile)
        last = dot(g_ref[rows, columns(masks[-1])], inner[columns(masks[-1]), :])
        power_t[:, rows] = (rough[rows, :] + last).astype(BF16).T
    one, two, three = pieces_of(inv1[...], 3)
    for at in range(0, depth, tile):
        rows = slice(at, at + tile)
        block_t = power_t[:, rows]
        once = dot(three, block_t) + dot(two, block_t) + dot(one, block_t)
        tops[:, rows], lows[:, rows] = pieces_of(once, 2)
    crossed = dot_t(tops[...], lows[...])
    gram[1, 0] = dot_t(tops[...], tops[...]) + (dot_t(lows[...], lows[...]) + (crossed + crossed.T))
    for item in spread:
        spread_copy(*item).wait_send()
    if len(peers) > 1:
        total_next(1)

    make2, absorb2 = halving(part2, land2, s_rs2, r_rs2)

    def cross_part(h, m):
        part2[h, m] = dot(power_t[h * half : (h + 1) * half, :], g_ref[:, columns(m)])

    def beside(phase):
        if phase == 0:
            for h, _, m, _ in schedule[0]:
                cross_part(h, m)
        if phase == bits - 1:
            for move in schedule[0]:
                make2(*move).start()
            started = [(move[0], move[2]) for move in schedule[0]]
            for h, m in [(h, m) for m in range(n) for h in range(2)]:
                if (h, m) not in started:
                    cross_part(h, m)
            for at in range(0, depth, tile):
                rows = slice(at, at + tile)
                top_rows[rows, :] = tops[:, rows].T
                low_rows[rows, :] = lows[:, rows].T

    gram_exchange(1, beside)
    for at in range(2, len(peers) - 1):
        total_next(at)
    work[...] = gram[1, bits]
    panel_steps(work, 0, panels // 2)
    forward(make2, absorb2)
    panel_steps(work, panels // 2, panels)
    inv2 = lower_of(work)
    high, low = pieces_of(inv2.T, 2)
    for at in range(0, depth, tile):
        rows = slice(at, at + tile)
        fresh = dot(low_rows[rows, :], high) + dot(top_rows[rows, :], low) + dot(top_rows[rows, :], high)
        fresh_ref[rows, :] = jnp.where(refresh, fresh, jnp.where(live, b_ref[rows, :].astype(F32), 0.0))
    both = dot(inv2, inv1[...], HIGHEST)
    if len(peers) > 2:
        total_next(len(peers) - 1)
    final = total[len(peers)]
    norm = lax.rsqrt(final[0:1, 0:1] / (final[1:2, 0:1] * entries) + 1e-6)
    finish(make2, absorb2)
    cross = jnp.concatenate([part2[0, 0], part2[1, 0]], axis=0)
    stale = jnp.concatenate([part[0, 0], part[1, 0]], axis=0)
    turned = dot(both, cross, HIGHEST)
    rot_ref[...] = jnp.where(refresh, turned, jnp.where(live, stale, 0.0)) * norm


def on_device(n, experts, grads, basis, loads, flags):
    _, depth, wide = grads.shape
    size = basis.shape[2]
    block = wide // n
    bits = n.bit_length() - 1
    peers = bits + experts.bit_length() - 1
    moves = 2 * (n - 1)
    live = loads
    refresh = jnp.where(loads >= 1, flags, 0)
    vmem = pl.BlockSpec(memory_space=pltpu.VMEM)
    smem = pl.BlockSpec(memory_space=pltpu.SMEM)
    chunk = (size // 2, block)
    dma = pltpu.SemaphoreType.DMA
    new_basis, rotated = pl.pallas_call(
        functools.partial(kernel, n, experts, float(depth * n * wide)),
        out_shape=(
            jax.ShapeDtypeStruct((depth, size), F32),
            jax.ShapeDtypeStruct((size, block), F32),
        ),
        in_specs=[pl.BlockSpec(memory_space=pl.ANY), vmem, smem, smem],
        out_specs=(vmem, vmem),
        scratch_shapes=[
            pltpu.VMEM((depth, wide), BF16),
            pltpu.SemaphoreType.DMA((n,)),
            pltpu.VMEM((size, depth), BF16),
            pltpu.VMEM((2, n, *chunk), F32),
            pltpu.VMEM((moves, *chunk), F32),
            pltpu.VMEM((2, n, *chunk), F32),
            pltpu.VMEM((moves, *chunk), F32),
            pltpu.VMEM((2, n, *chunk), F32),
            pltpu.VMEM((wide, size), BF16),
            pltpu.VMEM((size, depth), BF16),
            pltpu.VMEM((depth, size), F32),
            pltpu.VMEM((size, depth), BF16),
            pltpu.VMEM((size, depth), BF16),
            pltpu.VMEM((depth, size), BF16),
            pltpu.VMEM((depth, size), BF16),
            pltpu.VMEM((size, size), F32),
            pltpu.VMEM((size, size), F32),
            pltpu.VMEM((2, bits + 1, size, size), F32),
            pltpu.VMEM((2, bits, size, size), F32),
            pltpu.VMEM((peers + 1, 8, 128), F32),
            pltpu.VMEM((peers, 8, 128), F32),
            dma((moves,)), dma((moves,)), dma((moves,)), dma((moves,)), dma((moves,)), dma((moves,)),
            dma((2, bits, 2)), dma((2, bits, 2)), dma((peers,)), dma((peers,)),
        ],
        compiler_params=pltpu.CompilerParams(
            collective_id=0, has_side_effects=True, vmem_limit_bytes=58 * 1024 * 1024
        ),
    )(grads[0], basis[0], live, refresh)
    return new_basis[None], rotated[None]


def solution(mesh):
    placed = (P("expert", "row", None), P("expert", "row", None), P("expert"), P("expert"))
    return jax.shard_map(
        functools.partial(on_device, mesh.shape["row"], mesh.shape["expert"]),
        mesh=mesh,
        in_specs=placed,
        out_specs=(P("expert", "row", None), P("expert", None, "row")),
        check_vma=False,
    )
```
